32 devices in a mesh: gx: 4 (over y, core), gy: 2 (over x), gz: 4 (over z).
Axes of the slice: x: 2, y: 2, z: 4, core: 2. Of those that a mesh axis runs over, the one named last changes fastest.
Arguments:
- right_side: float32 [64, 1024, 256], P('gz', 'gx', 'gy'), may hold values from -8 to 8
- diagonal: float32 [64, 1024, 256], P('gz', 'gx', 'gy'), may hold values from 0.02 to 1
- regime: int32 [1024, 256], P('gx', 'gy'), may hold values from 0 to 7
- inverses: float32 [8, 64, 64], replicated, as said below
Outputs:
- solution: float32 [64, 1024, 256], P('gz', 'gx', 'gy')
- residual: float32 [64, 1024, 256], P('gz', 'gx', 'gy')
The draws below stay inside these ranges and needn't reach their ends.
Inputs may be any that keep to these rules, and one draw needn't show every extreme that they name: `inverses`: each block is symmetric positive definite.
All inputs are finite; a program needn't handle non-finite values.
Results may differ from the reference program's by a relative error of at most 0.00025.
Values sent between devices are 32-bit elements; how exact they have to be, the bound alone decides.
A program may use at most 128 MiB of HBM per device.

```python
import math
import jax
import jax.numpy as jnp
from jax import lax

NZ = 64
NREG = 8
ITERS = 3
NX = 1024
NY = 256


def draw_inverses(key, part):
    coeffs = jax.random.uniform(key, (NREG, NZ), jnp.float32, 2.3, 4.5)
    upper = jnp.eye(NZ, k=1, dtype=jnp.float32)
    lower = jnp.eye(NZ, k=-1, dtype=jnp.float32)
    tridiag = coeffs[:, :, None] * jnp.eye(NZ, dtype=jnp.float32)[None] - upper[None] - lower[None]
    inverted = jnp.linalg.inv(tridiag)
    return (0.5 * (inverted + jnp.swapaxes(inverted, 1, 2))).astype(jnp.float32)


def touch_ends(entries, rng, low, high):
    dims = entries.shape
    spot = [jax.random.randint(jax.random.fold_in(rng, axis), (), 0, dims[axis]) for axis in range(len(dims))]
    entries = entries.at[tuple(spot)].set(low)
    longest = dims.index(max(dims))
    spot[longest] = (spot[longest] + 1) % dims[longest]
    return entries.at[tuple(spot)].set(high)


def level_of(rng, shape, pieces, least, top_value):
    def one(axis_at, shards_of):
        draws = jax.random.uniform(jax.random.fold_in(jax.random.fold_in(rng, 6), axis_at), (shards_of,), jnp.float32, least / len(pieces), top_value / len(pieces))
        return jnp.repeat(jnp.exp(draws), shape[axis_at] // shards_of).reshape((-1,) + (1,) * (len(shape) - axis_at - 1))

    gain = one(*pieces[0])
    for cut in pieces[1:]:
        gain = gain * one(*cut)
    return gain


def bell_draw(stream_key, shape, deviation, limit, shards=(), kind=jnp.bfloat16):
    entries = jax.random.normal(stream_key, shape, jnp.float32) * deviation
    if len(shards) > 0:
        entries = level_of(stream_key, shape, shards, -0.22, 0.18) * entries
    return jnp.clip(entries, min=-limit, max=limit).astype(kind)


def setup_inputs(seed: int = 0) -> dict:
    arg_keys = jax.random.split(jax.random.key(seed), 5)
    return {
        "right_side": bell_draw(arg_keys[0], (NZ, NX, NY), 1.0, 8.0, ((0, 4), (1, 4), (2, 2)), jnp.float32),
        "diagonal": jnp.clip(jnp.exp(math.log(1.0) - 3.912023 * jax.random.uniform(arg_keys[1], (NZ, NX, NY), jnp.float32) ** level_of(arg_keys[1], (NZ, NX, NY), ((0, 4), (1, 4), (2, 2)), -0.2, 0.2)), 0.02, 1.0),
        "regime": touch_ends(jax.random.randint(arg_keys[2], (NX, NY), 0, NREG), jax.random.fold_in(arg_keys[2], 1), 0, NREG - 1).astype(jnp.int32),
        "inverses": draw_inverses(jax.random.fold_in(arg_keys[4], 71), 0),
    }


def operate(grid_field, diagonal):
    padded = jnp.pad(grid_field, 1)
    beside = padded[2:, 1:-1, 1:-1] + padded[:-2, 1:-1, 1:-1]
    beside = beside + padded[1:-1, 2:, 1:-1] + padded[1:-1, :-2, 1:-1]
    beside = beside + padded[1:-1, 1:-1, 2:] + padded[1:-1, 1:-1, :-2]
    return (6.0 + diagonal) * grid_field - beside

def precondition(grid_field, regime, inverses):
    flattened = grid_field.reshape(grid_field.shape[0], -1)
    chosen = regime.reshape(-1)
    result = jnp.zeros_like(flattened)
    for member in range(NREG):
        product = jnp.dot(inverses[member], flattened, precision=lax.Precision.HIGHEST)
        result = result + jnp.where(chosen[None, :] == member, product, jnp.zeros_like(product))
    return result.reshape(grid_field.shape)

def reference(right_side, diagonal, regime, inverses):
    solution = jnp.zeros_like(right_side)
    residual = right_side
    precond = precondition(residual, regime, inverses)
    inner_rz = jnp.sum(residual * precond)
    search = precond
    for iteration in range(ITERS):
        image = operate(search, diagonal)
        step_len = inner_rz / jnp.sum(search * image)
        solution = solution + step_len * search
        residual = residual - step_len * image
        if iteration + 1 < ITERS:
            precond = precondition(residual, regime, inverses)
            rz_next = jnp.sum(residual * precond)
            search = precond + rz_next / inner_rz * search
            inner_rz = rz_next
    return (solution, residual)
```

```python
import functools

import jax
import jax.numpy as jnp
from jax import lax
from jax.experimental import pallas as pl
from jax.experimental.pallas import tpu as pltpu
from jax.sharding import PartitionSpec as P

MESH = pl.DeviceIdType.MESH
BASIS = 3
CHUNKS = 4
SUMS = 16


def kernel(
    sizes,
    rhs,
    diag,
    regime,
    inverses,
    weights,
    x_out,
    r_out,
    rhs_z,
    diag_z,
    rhs_t,
    diag_t,
    fields,
    images,
    edges,
    edges_left,
    edges_right,
    x_z,
    r_z,
    sums_z,
    sums_x,
    sums_y,
    local_sem,
    in_send,
    in_recv,
    halo_send,
    halo_recv,
    sum_send,
    sum_recv,
    out_send,
    out_recv,
    out_local,
):
    nx, ny, nz = sizes["gx"], sizes["gy"], sizes["gz"]
    mx, my, mz = lax.axis_index("gx"), lax.axis_index("gy"), lax.axis_index("gz")
    slab = rhs.shape[0]
    depth = slab * nz
    rows = rhs.shape[1] // nz
    lanes = rhs.shape[2]
    nreg = inverses.shape[0]

    even = lax.rem(mx, 2) == 0

    def place(z):
        return jnp.where(even, z, nz - 1 - z)

    mine = place(mz)

    def row_span(z, start, count):
        return pl.ds(pl.multiple_of(place(z) * rows + start, 8), count)

    def slab_span(z):
        return pl.ds(z * slab, slab)

    axes = (("gx", nx, mx), ("gy", ny, my), ("gz", nz, mz))
    barrier = pltpu.get_barrier_semaphore()
    for name, count, me in axes:
        for k in range(1, count):
            pl.semaphore_signal(
                barrier, inc=1, device_id={name: lax.rem(me + k, count)}, device_id_type=MESH
            )
    pl.semaphore_wait(barrier, nx + ny + nz - 3)

    def slab_in(which, source, target, k, peer, span_owner):
        return pltpu.make_async_remote_copy(
            src_ref=source.at[:, row_span(peer, 0, rows), :],
            dst_ref=target.at[slab_span(span_owner)],
            send_sem=in_send.at[which, k],
            recv_sem=in_recv.at[which, k],
            device_id={"gz": peer},
            device_id_type=MESH,
        )

    pairs = ((rhs, rhs_z), (diag, diag_z))
    for which, (source, target) in enumerate(pairs):
        for k in (list(range(1, nz))):
            slab_in(which, source, target, k, lax.rem(mz + k, nz), mz).start()
        pltpu.make_async_copy(
            source.at[:, row_span(mz, 0, rows), :], target.at[slab_span(mz)], local_sem.at[which]
        ).start()

    def slab_wait(which):
        source, target = pairs[which]
        pltpu.make_async_copy(
            source.at[:, row_span(mz, 0, rows), :], target.at[slab_span(mz)], local_sem.at[which]
        ).wait()
        for k in range(1, nz):
            sender = lax.rem(mz + nz - k, nz)
            slab_in(which, source, target, k, sender, sender).wait_recv()

    blocks = inverses[...]
    scale = 1.0 / jnp.max(jnp.max(jnp.abs(blocks), axis=0), axis=(0, 1), keepdims=True)
    total = jnp.sum(blocks, axis=0)
    on_diagonal = lax.broadcasted_iota(jnp.int32, total.shape, 0) == lax.broadcasted_iota(
        jnp.int32, total.shape, 1
    )
    trace = jnp.sum(jnp.where(on_diagonal, total, 0.0), axis=(0, 1), keepdims=True)
    shift = scale * trace * (6.0 / (nreg * depth))

    lane = lax.broadcasted_iota(jnp.int32, (depth, lanes), 1)
    layer = lax.broadcasted_iota(jnp.int32, (depth, lanes), 0)
    zeros = jnp.zeros((depth, lanes), jnp.float32)

    has_prev = jnp.logical_or(mine > 0, mx > 0)
    has_next = jnp.logical_or(mine < nz - 1, mx < nx - 1)
    has_left = my > 0
    has_right = my < ny - 1
    step_z = jnp.where(even, 1, -1)
    at_top, at_end = mine == 0, mine == nz - 1
    prev_id = {
        "gx": jnp.where(at_top, jnp.maximum(mx - 1, 0), mx),
        "gz": jnp.where(at_top, mz, mz - step_z),
    }
    next_id = {
        "gx": jnp.where(at_end, jnp.minimum(mx + 1, nx - 1), mx),
        "gz": jnp.where(at_end, mz, mz + step_z),
    }
    left_id = {"gy": jnp.maximum(my - 1, 0)}
    right_id = {"gy": jnp.minimum(my + 1, ny - 1)}

    def halo(n):
        rows_of = fields.at[n]
        return (
            (has_prev, has_next, rows_of.at[1], rows_of.at[rows + 1], prev_id),
            (has_next, has_prev, rows_of.at[rows], rows_of.at[0], next_id),
            (has_left, has_right, edges.at[n], edges_right.at[n], left_id),
            (has_right, has_left, edges.at[n], edges_left.at[n], right_id),
        )

    def halo_copy(n, at, source, target, device):
        return pltpu.make_async_remote_copy(
            src_ref=source,
            dst_ref=target,
            send_sem=halo_send.at[n, at],
            recv_sem=halo_recv.at[n, at],
            device_id=device,
            device_id_type=MESH,
        )

    for n in range(BASIS):
        for _, gets, _, target, _ in halo(n):

            @pl.when(jnp.logical_not(gets))
            def _(target=target):
                target[...] = zeros

    def precondition(n):
        edges[n] = zeros

        def body(b, carry):
            columns = []
            for half in range(2):
                i = 2 * b + half
                if n == 0:
                    column = rhs_z.reshape(depth * rows, lanes)[pl.ds(i, depth, stride=rows), :]
                    rhs_t[i] = column
                else:
                    column = images[n - 1, i]
                columns.append(column)
            wide = jnp.concatenate(columns, axis=1)
            high = wide.astype(jnp.bfloat16)
            low = (wide - high.astype(jnp.float32)).astype(jnp.bfloat16)
            stacked = jnp.concatenate([high, high, low], axis=0)
            product = jnp.dot(weights[...], stacked, preferred_element_type=jnp.float32)
            packed = edges[n]
            for half in range(2):
                i = 2 * b + half
                chosen = jnp.broadcast_to(
                    regime[pl.ds(mine * rows + i, 1), :], (depth, lanes)
                )
                span = slice(half * lanes, (half + 1) * lanes)
                picked = product[:depth, span]
                for member in range(1, nreg):
                    part = product[member * depth : (member + 1) * depth, span]
                    picked = jnp.where(chosen == member, part, picked)
                value = picked * scale
                if n > 0:
                    value = value - shift * fields[n - 1, i + 1]
                fields[n, i + 1] = value
                packed = jnp.where(lane == i, pltpu.roll(value, i, 1), packed)
                packed = jnp.where(
                    lane == rows + i, pltpu.roll(value, lax.rem(rows + i + 1, lanes), 1), packed
                )
            edges[n] = packed
            return carry

        lax.fori_loop(0, rows // 2, body, 0)
        for at, (sends, _, source, target, device) in enumerate(halo(n)):

            @pl.when(sends)
            def _(at=at, source=source, target=target, device=device):
                halo_copy(n, at, source, target, device).start()

    def halo_wait(n):
        for at, (_, gets, source, target, device) in enumerate(halo(n)):

            @pl.when(gets)
            def _(at=at, source=source, target=target, device=device):
                halo_copy(n, at, source, target, device).wait_recv()

    def fold(product):
        return jnp.sum(product.reshape(depth // 8, 8, lanes), axis=0)

    def operate(n):
        halo_wait(n)

        def body(i, carry):
            field = fields[n, i + 1]
            if n == 0:
                bulk = diag_z.reshape(depth * rows, lanes)[pl.ds(i, depth, stride=rows), :]
                diag_t[i] = bulk
            else:
                bulk = diag_t[i]
            beside = fields[n, i] + fields[n, i + 2]
            beside = beside + jnp.where(layer == 0, 0.0, pltpu.roll(field, 1, 0))
            beside = beside + jnp.where(layer == depth - 1, 0.0, pltpu.roll(field, depth - 1, 0))
            from_left = pltpu.roll(edges_left[n], lanes - rows - i, 1)
            beside = beside + jnp.where(lane == 0, from_left, pltpu.roll(field, 1, 1))
            from_right = pltpu.roll(edges_right[n], lanes - 1 - i, 1)
            beside = beside + jnp.where(
                lane == lanes - 1, from_right, pltpu.roll(field, lanes - 1, 1)
            )
            image = (6.0 + bulk) * field - beside
            images[n, i] = image
            sums = [fold(rhs_t[i] * field), fold(field * image)]
            for m in range(n):
                sums.append(fold(fields[m, i + 1] * image))
            return tuple(old + new for old, new in zip(carry, sums))

        start = tuple(jnp.zeros((8, lanes), jnp.float32) for _ in range(n + 2))
        parts = lax.fori_loop(0, rows, body, start)
        return [jnp.sum(part, axis=0, keepdims=True) for part in parts]

    slab_wait(0)
    precondition(0)
    slab_wait(1)
    sums = operate(0)
    precondition(1)
    sums = sums + operate(1)
    precondition(2)
    sums = sums + operate(2)

    sums.append(jnp.zeros((SUMS - len(sums), lanes), jnp.float32))
    value = jnp.concatenate(sums, axis=0)
    stages = (("gz", nz, mz, sums_z), ("gx", nx, mx, sums_x), ("gy", ny, my, sums_y))
    for stage, (name, count, me, slots) in enumerate(stages):
        slots[me] = value

        def sum_copy(k, peer, owner):
            return pltpu.make_async_remote_copy(
                src_ref=slots.at[me],
                dst_ref=slots.at[owner],
                send_sem=sum_send.at[stage, k],
                recv_sem=sum_recv.at[stage, k],
                device_id={name: peer},
                device_id_type=MESH,
            )

        for k in range(1, count):
            sum_copy(k, lax.rem(me + k, count), me).start()
        for k in range(1, count):
            sender = lax.rem(me + count - k, count)
            sum_copy(k, sender, sender).wait_recv()
        value = slots[0]
        for at in range(1, count):
            value = value + slots[at]
        for k in range(1, count):
            sum_copy(k, lax.rem(me + k, count), me).wait_send()

    def entry(at):
        row = jnp.sum(value[at : at + 1, :], axis=1, keepdims=True)
        return jnp.broadcast_to(row, (8, lanes))

    g0, a00, g1, a11, a01, g2, a22, a02, a12 = [entry(at) for at in range(9)]

    def inverse(pivot, size):
        good = pivot > 1e-7 * size
        return jnp.where(good, 1.0 / jnp.where(good, pivot, 1.0), 0.0)

    p0 = inverse(a00, a00)
    l1, l2 = a01 * p0, a02 * p0
    d1 = a11 - l1 * a01
    e1 = a12 - l2 * a01
    h1 = g1 - l1 * g0
    p1 = inverse(d1, a11)
    l21 = e1 * p1
    d2 = a22 - l2 * a02 - l21 * e1
    h2 = g2 - l2 * g0 - l21 * h1
    c2 = h2 * inverse(d2, a22)
    c1 = (h1 - e1 * c2) * p1
    c0 = (g0 - a01 * c1 - a02 * c2) * p0
    c0, c1, c2 = (c[0:1] for c in (c0, c1, c2))

    piece = rows // CHUNKS
    outs = ((x_z, x_out), (r_z, r_out))

    def slab_out(which, chunk, k, peer, owner):
        source, target = outs[which]
        return pltpu.make_async_remote_copy(
            src_ref=source.at[slab_span(peer), pl.ds(chunk * piece, piece), :],
            dst_ref=target.at[:, row_span(owner, chunk * piece, piece), :],
            send_sem=out_send.at[which, chunk, k],
            recv_sem=out_recv.at[which, chunk, k],
            device_id={"gz": peer},
            device_id_type=MESH,
        )

    def keep(which, chunk):
        source, target = outs[which]
        return pltpu.make_async_copy(
            source.at[slab_span(mz), pl.ds(chunk * piece, piece), :],
            target.at[:, row_span(mz, chunk * piece, piece), :],
            out_local.at[which, chunk],
        )

    for chunk in range(CHUNKS):

        def final(i, carry):
            i = chunk * piece + i
            span = pl.ds(i, depth, stride=rows)
            x = c0 * fields[0, i + 1] + c1 * fields[1, i + 1] + c2 * fields[2, i + 1]
            x_z.reshape(depth * rows, lanes)[span, :] = x
            r = rhs_t[i] - (c0 * images[0, i] + c1 * images[1, i] + c2 * images[2, i])
            r_z.reshape(depth * rows, lanes)[span, :] = r
            return carry

        lax.fori_loop(0, piece, final, 0)
        for which in range(2):
            for k in range(1, nz):
                slab_out(which, chunk, k, lax.rem(mz + k, nz), mz).start()
            keep(which, chunk).start()

    for which, (source, target) in enumerate(pairs):
        for k in range(1, nz):
            slab_in(which, source, target, k, lax.rem(mz + k, nz), mz).wait_send()
    for n in range(BASIS):
        for at, (sends, _, source, target, device) in enumerate(halo(n)):

            @pl.when(sends)
            def _(n=n, at=at, source=source, target=target, device=device):
                halo_copy(n, at, source, target, device).wait_send()

    for which in range(2):
        for chunk in range(CHUNKS):
            keep(which, chunk).wait()
            for k in range(1, nz):
                sender = lax.rem(mz + nz - k, nz)
                slab_out(which, chunk, k, sender, sender).wait_recv()
                slab_out(which, chunk, k, lax.rem(mz + k, nz), mz).wait_send()


def per_device(sizes, right_side, diagonal, regime, inverses):
    slab, wide, lanes = right_side.shape
    nz = sizes["gz"]
    depth, rows = slab * nz, wide // nz
    nreg = inverses.shape[0]
    high = lax.reduce_precision(inverses, 8, 7)
    low = lax.reduce_precision(inverses - high, 8, 7)
    weights = jnp.concatenate([high, low, high], axis=-1).reshape(nreg * depth, 3 * depth)
    weights = weights.astype(jnp.bfloat16)
    column = (rows, depth, lanes)
    layered = (depth, rows, lanes)
    f32 = jnp.float32
    dma = pltpu.SemaphoreType.DMA
    return pl.pallas_call(
        functools.partial(kernel, sizes),
        out_shape=[jax.ShapeDtypeStruct(right_side.shape, f32)] * 2,
        in_specs=[pl.BlockSpec(memory_space=pl.ANY)] * 2
        + [pl.BlockSpec(memory_space=pltpu.VMEM)] * 3,
        out_specs=[pl.BlockSpec(memory_space=pl.ANY)] * 2,
        scratch_shapes=[
            pltpu.VMEM(layered, f32),
            pltpu.VMEM(layered, f32),
            pltpu.VMEM(column, f32),
            pltpu.VMEM(column, f32),
            pltpu.VMEM((BASIS, rows + 2, depth, lanes), f32),
            pltpu.VMEM((BASIS, rows, depth, lanes), f32),
            pltpu.VMEM((BASIS, depth, lanes), f32),
            pltpu.VMEM((BASIS, depth, lanes), f32),
            pltpu.VMEM((BASIS, depth, lanes), f32),
            pltpu.VMEM(layered, f32),
            pltpu.VMEM(layered, f32),
            pltpu.VMEM((nz, SUMS, lanes), f32),
            pltpu.VMEM((sizes["gx"], SUMS, lanes), f32),
            pltpu.VMEM((sizes["gy"], SUMS, lanes), f32),
            dma((2,)),
            dma((2, nz)),
            dma((2, nz)),
            dma((BASIS, 4)),
            dma((BASIS, 4)),
            dma((3, max(sizes.values()))),
            dma((3, max(sizes.values()))),
            dma((2, CHUNKS, nz)),
            dma((2, CHUNKS, nz)),
            dma((2, CHUNKS)),
        ],
        compiler_params=pltpu.CompilerParams(
            collective_id=0, has_side_effects=True, vmem_limit_bytes=56 * 1024 * 1024
        ),
    )(right_side, diagonal, regime, inverses, weights)


def solution(mesh):
    sizes = {name: mesh.shape[name] for name in ("gx", "gy", "gz")}
    in_specs = (P("gz", "gx", "gy"), P("gz", "gx", "gy"), P("gx", "gy"), P())
    out_specs = (P("gz", "gx", "gy"), P("gz", "gx", "gy"))
    return jax.shard_map(
        functools.partial(per_device, sizes),
        mesh=mesh,
        in_specs=in_specs,
        out_specs=out_specs,
        check_vma=False,
    )
```

```python
import functools

import jax
import jax.numpy as jnp
from jax import lax
from jax.experimental import pallas as pl
from jax.experimental.pallas import tpu as pltpu
from jax.sharding import PartitionSpec as P

MESH = pl.DeviceIdType.MESH
BASIS = 3
CHUNKS = 4
SUMS = 16
UNROLL_M = 2
UNROLL_A = 4
UNROLL_F = 4


def kernel(
    sizes,
    rhs,
    diag,
    regime,
    inverses,
    x_out,
    r_out,
    weights,
    rhs_z,
    diag_z,
    rhs_slab,
    diag_slab,
    rhs_t,
    diag_t,
    fields,
    images,
    edges,
    edges_left,
    edges_right,
    x_z,
    x_rim,
    x_in,
    rim_in,
    r_in,
    sums_z,
    sums_x,
    sums_y,
    local_sem,
    in_send,
    in_recv,
    halo_send,
    halo_recv,
    sum_send,
    sum_recv,
    out_send,
    out_recv,
    out_local,
    rim_send,
    rim_recv,
    slab_sem,
):
    nx, ny, nz = sizes["gx"], sizes["gy"], sizes["gz"]
    mx, my, mz = lax.axis_index("gx"), lax.axis_index("gy"), lax.axis_index("gz")
    slab = rhs.shape[0]
    depth = slab * nz
    rows = rhs.shape[1] // nz
    lanes = rhs.shape[2]
    nreg = inverses.shape[0]

    even = lax.rem(mx, 2) == 0

    def place(z):
        return jnp.where(even, z, nz - 1 - z)

    mine = place(mz)

    def row_span(z, start, count):
        return pl.ds(pl.multiple_of(place(z) * rows + start, 8), count)

    def slab_span(z):
        return pl.ds(z * slab, slab)

    axes = (("gx", nx, mx), ("gy", ny, my), ("gz", nz, mz))
    barrier = pltpu.get_barrier_semaphore()
    for name, count, me in axes:
        for k in range(1, count):
            pl.semaphore_signal(
                barrier, inc=1, device_id={name: lax.rem(me + k, count)}, device_id_type=MESH
            )
    pl.semaphore_wait(barrier, nx + ny + nz - 3)

    piece = rows // CHUNKS
    pairs = ((rhs, rhs_z), (diag, diag_z))

    def slab_in(which, chunk, k, peer, owner):
        source, target = pairs[which]
        return pltpu.make_async_remote_copy(
            src_ref=source.at[:, row_span(peer, chunk * piece, piece), :],
            dst_ref=target.at[slab_span(owner), pl.ds(chunk * piece, piece), :],
            send_sem=in_send.at[which, chunk, k],
            recv_sem=in_recv.at[which, chunk, k],
            device_id={"gz": peer},
            device_id_type=MESH,
        )

    def own_in(which):
        source, target = pairs[which]
        return pltpu.make_async_copy(
            source.at[:, row_span(mz, 0, rows), :], target.at[slab_span(mz)], local_sem.at[which]
        )

    slabs = ((rhs, rhs_slab), (diag, diag_slab))
    for which in range(2):
        for chunk in range(CHUNKS):
            for k in range(1, nz):
                slab_in(which, chunk, k, lax.rem(mz + k, nz), mz).start()
        own_in(which).start()
    for which, (source, target) in enumerate(slabs):
        pltpu.make_async_copy(source, target, slab_sem.at[which]).start()

    def slab_wait(which, chunk):
        if chunk == 0:
            own_in(which).wait()
        for k in range(1, nz):
            sender = lax.rem(mz + nz - k, nz)
            slab_in(which, chunk, k, sender, sender).wait_recv()

    for member in range(nreg):
        block = inverses[member]
        high = block.astype(jnp.bfloat16).astype(jnp.float32)
        split = jnp.concatenate([high, block - high, high], axis=1)
        weights[member * depth : (member + 1) * depth, :] = split.astype(jnp.bfloat16)

    blocks = inverses[...]
    scale = 1.0 / jnp.max(jnp.max(jnp.abs(blocks), axis=0), axis=(0, 1), keepdims=True)
    total = jnp.sum(blocks, axis=0)
    on_diagonal = lax.broadcasted_iota(jnp.int32, total.shape, 0) == lax.broadcasted_iota(
        jnp.int32, total.shape, 1
    )
    trace = jnp.sum(jnp.where(on_diagonal, total, 0.0), axis=(0, 1), keepdims=True)
    shift = scale * trace * (6.0 / (nreg * depth))

    lane = lax.broadcasted_iota(jnp.int32, (depth, lanes), 1)
    layer = lax.broadcasted_iota(jnp.int32, (depth, lanes), 0)
    zeros = jnp.zeros((depth, lanes), jnp.float32)

    has_prev = jnp.logical_or(mine > 0, mx > 0)
    has_next = jnp.logical_or(mine < nz - 1, mx < nx - 1)
    has_left = my > 0
    has_right = my < ny - 1
    step_z = jnp.where(even, 1, -1)
    at_top, at_end = mine == 0, mine == nz - 1
    prev_id = {
        "gx": jnp.where(at_top, jnp.maximum(mx - 1, 0), mx),
        "gz": jnp.where(at_top, mz, mz - step_z),
    }
    next_id = {
        "gx": jnp.where(at_end, jnp.minimum(mx + 1, nx - 1), mx),
        "gz": jnp.where(at_end, mz, mz + step_z),
    }
    left_id = {"gy": jnp.maximum(my - 1, 0)}
    right_id = {"gy": jnp.minimum(my + 1, ny - 1)}

    def halo(n):
        rows_of = fields.at[n]
        return (
            (has_prev, has_next, rows_of.at[1], rows_of.at[rows + 1], prev_id),
            (has_next, has_prev, rows_of.at[rows], rows_of.at[0], next_id),
            (has_left, has_right, edges.at[n], edges_right.at[n], left_id),
            (has_right, has_left, edges.at[n], edges_left.at[n], right_id),
        )

    def halo_copy(n, at, source, target, device):
        return pltpu.make_async_remote_copy(
            src_ref=source,
            dst_ref=target,
            send_sem=halo_send.at[n, at],
            recv_sem=halo_recv.at[n, at],
            device_id=device,
            device_id_type=MESH,
        )

    for n in range(BASIS):
        for _, gets, _, target, _ in halo(n):

            @pl.when(jnp.logical_not(gets))
            def _(target=target):
                target[...] = zeros

    def precondition(n):
        edges[n] = zeros

        def body(b, carry):
            columns = []
            for half in range(2):
                i = 2 * b + half
                if n == 0:
                    column = rhs_z.reshape(depth * rows, lanes)[pl.ds(i, depth, stride=rows), :]
                    rhs_t[i] = column
                else:
                    column = images[n - 1, i]
                columns.append(column)
            wide = jnp.concatenate(columns, axis=1)
            high = wide.astype(jnp.bfloat16)
            low = (wide - high.astype(jnp.float32)).astype(jnp.bfloat16)
            stacked = jnp.concatenate([high, high, low], axis=0)
            product = jnp.dot(weights[...], stacked, preferred_element_type=jnp.float32)
            packed = edges[n]
            for half in range(2):
                i = 2 * b + half
                chosen = jnp.broadcast_to(
                    regime[pl.ds(mine * rows + i, 1), :], (depth, lanes)
                )
                span = slice(half * lanes, (half + 1) * lanes)
                picked = product[:depth, span]
                for member in range(1, nreg):
                    part = product[member * depth : (member + 1) * depth, span]
                    picked = jnp.where(chosen == member, part, picked)
                value = picked * scale
                if n > 0:
                    value = value - shift * fields[n - 1, i + 1]
                fields[n, i + 1] = value
                packed = jnp.where(lane == i, pltpu.roll(value, i, 1), packed)
                packed = jnp.where(
                    lane == rows + i, pltpu.roll(value, lax.rem(rows + i + 1, lanes), 1), packed
                )
            edges[n] = packed
            return carry

        turns = piece // (2 * UNROLL_M)
        for chunk in range(CHUNKS):
            if n == 0:
                slab_wait(0, chunk)

            def turn(t, carry, chunk=chunk):
                for u in range(UNROLL_M):
                    body(chunk * (piece // 2) + t * UNROLL_M + u, carry)
                return carry

            lax.fori_loop(0, turns, turn, 0)
        for at, (sends, _, source, target, device) in enumerate(halo(n)):

            @pl.when(sends)
            def _(at=at, source=source, target=target, device=device):
                halo_copy(n, at, source, target, device).start()

    def halo_wait(n):
        for at, (_, gets, source, target, device) in enumerate(halo(n)):

            @pl.when(gets)
            def _(at=at, source=source, target=target, device=device):
                halo_copy(n, at, source, target, device).wait_recv()

    def fold(product):
        return jnp.sum(product.reshape(depth // 8, 8, lanes), axis=0)

    def operate(n):
        halo_wait(n)

        def body(i, carry):
            field = fields[n, i + 1]
            if n == 0:
                bulk = diag_z.reshape(depth * rows, lanes)[pl.ds(i, depth, stride=rows), :]
                diag_t[i] = bulk
            else:
                bulk = diag_t[i]
            beside = fields[n, i] + fields[n, i + 2]
            beside = beside + jnp.where(layer == 0, 0.0, pltpu.roll(field, 1, 0))
            beside = beside + jnp.where(layer == depth - 1, 0.0, pltpu.roll(field, depth - 1, 0))
            from_left = pltpu.roll(edges_left[n], lanes - rows - i, 1)
            beside = beside + jnp.where(lane == 0, from_left, pltpu.roll(field, 1, 1))
            from_right = pltpu.roll(edges_right[n], lanes - 1 - i, 1)
            beside = beside + jnp.where(
                lane == lanes - 1, from_right, pltpu.roll(field, lanes - 1, 1)
            )
            image = (6.0 + bulk) * field - beside
            images[n, i] = image
            sums = [fold(rhs_t[i] * field), fold(field * image)]
            for m in range(n):
                sums.append(fold(fields[m, i + 1] * image))
            return tuple(old + new for old, new in zip(carry, sums))

        start = tuple(jnp.zeros((8, lanes), jnp.float32) for _ in range(n + 2))
        parts = start
        for chunk in range(CHUNKS):
            if n == 0:
                slab_wait(1, chunk)

            def turn(t, carry, chunk=chunk):
                for u in range(UNROLL_A):
                    carry = body(chunk * piece + t * UNROLL_A + u, carry)
                return carry

            parts = lax.fori_loop(0, piece // UNROLL_A, turn, parts)
        return [jnp.sum(part, axis=0, keepdims=True) for part in parts]

    precondition(0)
    sums = operate(0)
    precondition(1)
    sums = sums + operate(1)
    precondition(2)
    sums = sums + operate(2)

    sums.append(jnp.zeros((SUMS - len(sums), lanes), jnp.float32))
    value = jnp.concatenate(sums, axis=0)
    stages = (("gz", nz, mz, sums_z), ("gx", nx, mx, sums_x), ("gy", ny, my, sums_y))
    for stage, (name, count, me, slots) in enumerate(stages):
        slots[me] = value

        def sum_copy(k, peer, owner):
            return pltpu.make_async_remote_copy(
                src_ref=slots.at[me],
                dst_ref=slots.at[owner],
                send_sem=sum_send.at[stage, k],
                recv_sem=sum_recv.at[stage, k],
                device_id={name: peer},
                device_id_type=MESH,
            )

        for k in range(1, count):
            sum_copy(k, lax.rem(me + k, count), me).start()
        for k in range(1, count):
            sender = lax.rem(me + count - k, count)
            sum_copy(k, sender, sender).wait_recv()
        value = slots[0]
        for at in range(1, count):
            value = value + slots[at]
        for k in range(1, count):
            sum_copy(k, lax.rem(me + k, count), me).wait_send()

    def entry(at):
        row = jnp.sum(value[at : at + 1, :], axis=1, keepdims=True)
        return jnp.broadcast_to(row, (8, lanes))

    g0, a00, g1, a11, a01, g2, a22, a02, a12 = [entry(at) for at in range(9)]

    def inverse(pivot, size):
        good = pivot > 1e-7 * size
        return jnp.where(good, 1.0 / jnp.where(good, pivot, 1.0), 0.0)

    p0 = inverse(a00, a00)
    l1, l2 = a01 * p0, a02 * p0
    d1 = a11 - l1 * a01
    e1 = a12 - l2 * a01
    h1 = g1 - l1 * g0
    p1 = inverse(d1, a11)
    l21 = e1 * p1
    d2 = a22 - l2 * a02 - l21 * e1
    h2 = g2 - l2 * g0 - l21 * h1
    c2 = h2 * inverse(d2, a22)
    c1 = (h1 - e1 * c2) * p1
    c0 = (g0 - a01 * c1 - a02 * c2) * p0
    c0, c1, c2 = (c[0:1] for c in (c0, c1, c2))

    def mix(terms):
        first, second, third = terms
        return c0 * first + c1 * second + c2 * third

    x_rim[0] = mix([fields[n, 0] for n in range(BASIS)])
    x_rim[1] = mix([fields[n, rows + 1] for n in range(BASIS)])
    x_rim[2] = mix([edges_left[n] for n in range(BASIS)])
    x_rim[3] = mix([edges_right[n] for n in range(BASIS)])
    x_z[0] = jnp.zeros((rows, lanes), jnp.float32)
    x_z[depth + 1] = jnp.zeros((rows, lanes), jnp.float32)

    def rim_out(k, peer, owner):
        return pltpu.make_async_remote_copy(
            src_ref=x_rim.at[:, slab_span(peer), :],
            dst_ref=rim_in.at[owner],
            send_sem=rim_send.at[k],
            recv_sem=rim_recv.at[k],
            device_id={"gz": peer},
            device_id_type=MESH,
        )

    def slab_out(chunk, k, peer, owner):
        return pltpu.make_async_remote_copy(
            src_ref=x_z.at[pl.ds(peer * slab, slab + 2), pl.ds(chunk * piece, piece), :],
            dst_ref=x_in.at[owner, :, pl.ds(chunk * piece, piece), :],
            send_sem=out_send.at[chunk, k],
            recv_sem=out_recv.at[chunk, k],
            device_id={"gz": peer},
            device_id_type=MESH,
        )

    for chunk in range(CHUNKS):

        def final(t, carry):
            for u in range(UNROLL_F):
                i = chunk * piece + t * UNROLL_F + u
                x = mix([fields[n, i + 1] for n in range(BASIS)])
                x_z.reshape((depth + 2) * rows, lanes)[pl.ds(rows + i, depth, stride=rows), :] = x
            return carry

        lax.fori_loop(0, piece // UNROLL_F, final, 0)
        for k in range(1, nz):
            slab_out(chunk, k, lax.rem(mz + k, nz), mz).start()
    for k in range(1, nz):
        rim_out(k, lax.rem(mz + k, nz), mz).start()

    own_x = pltpu.make_async_copy(
        x_z.at[pl.ds(mz * slab, slab + 2)], x_in.at[mz], local_sem.at[0]
    )
    own_rim = pltpu.make_async_copy(
        x_rim.at[:, slab_span(mz), :], rim_in.at[mz], local_sem.at[1]
    )
    own_x.start()
    own_rim.start()
    for which, (source, target) in enumerate(slabs):
        pltpu.make_async_copy(source, target, slab_sem.at[which]).wait()
    for which in range(2):
        for chunk in range(CHUNKS):
            for k in range(1, nz):
                slab_in(which, chunk, k, lax.rem(mz + k, nz), mz).wait_send()
    for n in range(BASIS):
        for at, (sends, _, source, target, device) in enumerate(halo(n)):

            @pl.when(sends)
            def _(n=n, at=at, source=source, target=target, device=device):
                halo_copy(n, at, source, target, device).wait_send()

    plane_lane = lax.broadcasted_iota(jnp.int32, (rows, lanes), 1)
    plane_row = lax.broadcasted_iota(jnp.int32, (rows, lanes), 0)

    def result(which, owner):
        source = x_in.at[owner, pl.ds(1, slab)] if which == 0 else r_in.at[owner]
        return pltpu.make_async_copy(
            source,
            (x_out, r_out)[which].at[:, row_span(owner, 0, rows), :],
            out_local.at[which, owner],
        )

    def finish(owner):
        result(0, owner).start()
        rim = [rim_in[owner, 2], rim_in[owner, 3]]
        rim.append(jnp.zeros((lanes - 2 * slab, lanes), jnp.float32))
        turned = jnp.concatenate(rim, axis=0).T
        first, last = turned[rows : 2 * rows], turned[:rows]
        start = pl.multiple_of(place(owner) * rows, 8)

        def plane(z, carry):
            x = x_in[owner, z + 1]
            beside = x_in[owner, z] + x_in[owner, z + 2]
            above = jnp.broadcast_to(rim_in[owner, 0, pl.ds(z, 1), :], x.shape)
            below = jnp.broadcast_to(rim_in[owner, 1, pl.ds(z, 1), :], x.shape)
            beside = beside + jnp.where(plane_row == 0, above, pltpu.roll(x, 1, 0))
            beside = beside + jnp.where(plane_row == rows - 1, below, pltpu.roll(x, rows - 1, 0))
            from_left = pltpu.roll(first, lax.rem(lanes - z, lanes), 1)
            from_right = pltpu.roll(last, lanes - 1 - slab - z, 1)
            beside = beside + jnp.where(plane_lane == 0, from_left, pltpu.roll(x, 1, 1))
            beside = beside + jnp.where(
                plane_lane == lanes - 1, from_right, pltpu.roll(x, lanes - 1, 1)
            )
            image = (6.0 + diag_slab[z, pl.ds(start, rows), :]) * x - beside
            r_in[owner, z] = rhs_slab[z, pl.ds(start, rows), :] - image
            return carry

        def turn(t, carry):
            for u in range(UNROLL_F):
                carry = plane(t * UNROLL_F + u, carry)
            return carry

        lax.fori_loop(0, slab // UNROLL_F, turn, 0)
        result(1, owner).start()

    own_x.wait()
    own_rim.wait()
    finish(mz)
    order = sorted(range(1, nz), key=lambda k: (min(k, nz - k), k))
    for k in order:
        sender = lax.rem(mz + nz - k, nz)
        rim_out(k, sender, sender).wait_recv()
        for chunk in range(CHUNKS):
            slab_out(chunk, k, sender, sender).wait_recv()
        finish(sender)
    for k in range(nz):
        for which in range(2):
            result(which, lax.rem(mz + k, nz)).wait()
    for k in range(1, nz):
        peer = lax.rem(mz + k, nz)
        rim_out(k, peer, mz).wait_send()
        for chunk in range(CHUNKS):
            slab_out(chunk, k, peer, mz).wait_send()


def per_device(sizes, right_side, diagonal, regime, inverses):
    slab, wide, lanes = right_side.shape
    nz = sizes["gz"]
    depth, rows = slab * nz, wide // nz
    nreg = inverses.shape[0]
    column = (rows, depth, lanes)
    layered = (depth, rows, lanes)
    f32 = jnp.float32
    dma = pltpu.SemaphoreType.DMA
    return pl.pallas_call(
        functools.partial(kernel, sizes),
        out_shape=[jax.ShapeDtypeStruct(right_side.shape, f32)] * 2,
        in_specs=[pl.BlockSpec(memory_space=pl.ANY)] * 2
        + [pl.BlockSpec(memory_space=pltpu.VMEM)] * 2,
        out_specs=[pl.BlockSpec(memory_space=pl.ANY)] * 2,
        scratch_shapes=[
            pltpu.VMEM((nreg * depth, 3 * depth), jnp.bfloat16),
            pltpu.VMEM(layered, f32),
            pltpu.VMEM(layered, f32),
            pltpu.VMEM(right_side.shape, f32),
            pltpu.VMEM(right_side.shape, f32),
            pltpu.VMEM(column, f32),
            pltpu.VMEM(column, f32),
            pltpu.VMEM((BASIS, rows + 2, depth, lanes), f32),
            pltpu.VMEM((BASIS, rows, depth, lanes), f32),
            pltpu.VMEM((BASIS, depth, lanes), f32),
            pltpu.VMEM((BASIS, depth, lanes), f32),
            pltpu.VMEM((BASIS, depth, lanes), f32),
            pltpu.VMEM((depth + 2, rows, lanes), f32),
            pltpu.VMEM((4, depth, lanes), f32),
            pltpu.VMEM((nz, slab + 2, rows, lanes), f32),
            pltpu.VMEM((nz, 4, slab, lanes), f32),
            pltpu.VMEM((nz, slab, rows, lanes), f32),
            pltpu.VMEM((nz, SUMS, lanes), f32),
            pltpu.VMEM((sizes["gx"], SUMS, lanes), f32),
            pltpu.VMEM((sizes["gy"], SUMS, lanes), f32),
            dma((2,)),
            dma((2, CHUNKS, nz)),
            dma((2, CHUNKS, nz)),
            dma((BASIS, 4)),
            dma((BASIS, 4)),
            dma((3, max(sizes.values()))),
            dma((3, max(sizes.values()))),
            dma((CHUNKS, nz)),
            dma((CHUNKS, nz)),
            dma((2, nz)),
            dma((nz,)),
            dma((nz,)),
            dma((2,)),
        ],
        compiler_params=pltpu.CompilerParams(
            collective_id=0, has_side_effects=True, vmem_limit_bytes=56 * 1024 * 1024
        ),
    )(right_side, diagonal, regime, inverses)


def solution(mesh):
    sizes = {name: mesh.shape[name] for name in ("gx", "gy", "gz")}
    in_specs = (P("gz", "gx", "gy"), P("gz", "gx", "gy"), P("gx", "gy"), P())
    out_specs = (P("gz", "gx", "gy"), P("gz", "gx", "gy"))
    return jax.shard_map(
        functools.partial(per_device, sizes),
        mesh=mesh,
        in_specs=in_specs,
        out_specs=out_specs,
        check_vma=False,
    )
```

```python
import functools

import jax
import jax.numpy as jnp
from jax import lax
from jax.experimental import pallas as pl
from jax.experimental.pallas import tpu as pltpu
from jax.sharding import PartitionSpec as P

MESH = pl.DeviceIdType.MESH
BASIS = 3
CHUNKS = 4
SUMS = 16
UNROLL_M = 4
UNROLL_A = 8
UNROLL_F = 4


def kernel(
    sizes,
    rhs,
    diag,
    regime,
    inverses,
    x_out,
    r_out,
    weights,
    rhs_z,
    diag_z,
    rhs_slab,
    diag_slab,
    rhs_t,
    diag_t,
    fields,
    images,
    edges,
    edges_left,
    edges_right,
    x_z,
    x_rim,
    x_in,
    rim_in,
    r_in,
    sums_z,
    sums_x,
    sums_y,
    local_sem,
    in_send,
    in_recv,
    halo_send,
    halo_recv,
    sum_send,
    sum_recv,
    out_send,
    out_recv,
    out_local,
    rim_send,
    rim_recv,
    slab_sem,
):
    nx, ny, nz = sizes["gx"], sizes["gy"], sizes["gz"]
    mx, my, mz = lax.axis_index("gx"), lax.axis_index("gy"), lax.axis_index("gz")
    slab = rhs.shape[0]
    depth = slab * nz
    rows = rhs.shape[1] // nz
    lanes = rhs.shape[2]
    nreg = inverses.shape[0]

    even = lax.rem(mx, 2) == 0

    def place(z):
        return jnp.where(even, z, nz - 1 - z)

    mine = place(mz)

    def row_span(z, start, count):
        return pl.ds(pl.multiple_of(place(z) * rows + start, 8), count)

    def slab_span(z):
        return pl.ds(z * slab, slab)

    axes = (("gx", nx, mx), ("gy", ny, my), ("gz", nz, mz))
    barrier = pltpu.get_barrier_semaphore()
    for name, count, me in axes:
        for k in range(1, count):
            pl.semaphore_signal(
                barrier, inc=1, device_id={name: lax.rem(me + k, count)}, device_id_type=MESH
            )
    pl.semaphore_wait(barrier, nx + ny + nz - 3)

    piece = rows // CHUNKS
    pairs = ((rhs, rhs_z), (diag, diag_z))

    def slab_in(which, chunk, k, peer, owner):
        source, target = pairs[which]
        return pltpu.make_async_remote_copy(
            src_ref=source.at[:, row_span(peer, chunk * piece, piece), :],
            dst_ref=target.at[slab_span(owner), pl.ds(chunk * piece, piece), :],
            send_sem=in_send.at[which, chunk, k],
            recv_sem=in_recv.at[which, chunk, k],
            device_id={"gz": peer},
            device_id_type=MESH,
        )

    def own_in(which):
        source, target = pairs[which]
        return pltpu.make_async_copy(
            source.at[:, row_span(mz, 0, rows), :], target.at[slab_span(mz)], local_sem.at[which]
        )

    slabs = ((rhs, rhs_slab), (diag, diag_slab))
    for which in range(2):
        for chunk in range(CHUNKS):
            for k in range(1, nz):
                slab_in(which, chunk, k, lax.rem(mz + k, nz), mz).start()
        own_in(which).start()
    for which, (source, target) in enumerate(slabs):
        pltpu.make_async_copy(source, target, slab_sem.at[which]).start()

    def slab_wait(which, chunk):
        if chunk == 0:
            own_in(which).wait()
        for k in range(1, nz):
            sender = lax.rem(mz + nz - k, nz)
            slab_in(which, chunk, k, sender, sender).wait_recv()

    for member in range(nreg):
        block = inverses[member]
        high = block.astype(jnp.bfloat16).astype(jnp.float32)
        split = jnp.concatenate([high, block - high, high], axis=1)
        weights[member * depth : (member + 1) * depth, :] = split.astype(jnp.bfloat16)

    blocks = inverses[...]
    scale = 1.0 / jnp.max(jnp.max(jnp.abs(blocks), axis=0), axis=(0, 1), keepdims=True)
    total = jnp.sum(blocks, axis=0)
    on_diagonal = lax.broadcasted_iota(jnp.int32, total.shape, 0) == lax.broadcasted_iota(
        jnp.int32, total.shape, 1
    )
    trace = jnp.sum(jnp.where(on_diagonal, total, 0.0), axis=(0, 1), keepdims=True)
    shift = scale * trace * (6.0 / (nreg * depth))

    lane = lax.broadcasted_iota(jnp.int32, (depth, lanes), 1)
    layer = lax.broadcasted_iota(jnp.int32, (depth, lanes), 0)
    zeros = jnp.zeros((depth, lanes), jnp.float32)

    has_prev = jnp.logical_or(mine > 0, mx > 0)
    has_next = jnp.logical_or(mine < nz - 1, mx < nx - 1)
    has_left = my > 0
    has_right = my < ny - 1
    step_z = jnp.where(even, 1, -1)
    at_top, at_end = mine == 0, mine == nz - 1
    prev_id = {
        "gx": jnp.where(at_top, jnp.maximum(mx - 1, 0), mx),
        "gz": jnp.where(at_top, mz, mz - step_z),
    }
    next_id = {
        "gx": jnp.where(at_end, jnp.minimum(mx + 1, nx - 1), mx),
        "gz": jnp.where(at_end, mz, mz + step_z),
    }
    left_id = {"gy": jnp.maximum(my - 1, 0)}
    right_id = {"gy": jnp.minimum(my + 1, ny - 1)}

    def halo(n):
        rows_of = fields.at[n]
        return (
            (has_prev, has_next, rows_of.at[1], rows_of.at[rows + 1], prev_id),
            (has_next, has_prev, rows_of.at[rows], rows_of.at[0], next_id),
            (has_left, has_right, edges.at[n], edges_right.at[n], left_id),
            (has_right, has_left, edges.at[n], edges_left.at[n], right_id),
        )

    def halo_copy(n, at, source, target, device):
        return pltpu.make_async_remote_copy(
            src_ref=source,
            dst_ref=target,
            send_sem=halo_send.at[n, at],
            recv_sem=halo_recv.at[n, at],
            device_id=device,
            device_id_type=MESH,
        )

    for n in range(BASIS):
        for _, gets, _, target, _ in halo(n):

            @pl.when(jnp.logical_not(gets))
            def _(target=target):
                target[...] = zeros

    def precondition(n, chunks, done):
        if chunks[0] == 0:
            edges[n] = zeros

        def body(b, carry):
            columns = []
            for half in range(2):
                i = 2 * b + half
                if n == 0:
                    column = rhs_z.reshape(depth * rows, lanes)[pl.ds(i, depth, stride=rows), :]
                    rhs_t[i] = column
                else:
                    column = images[n - 1, i]
                columns.append(column)
            wide = jnp.concatenate(columns, axis=1)
            high = wide.astype(jnp.bfloat16)
            low = (wide - high.astype(jnp.float32)).astype(jnp.bfloat16)
            stacked = jnp.concatenate([high, high, low], axis=0)
            product = jnp.dot(weights[...], stacked, preferred_element_type=jnp.float32)
            packed = edges[n]
            for half in range(2):
                i = 2 * b + half
                chosen = jnp.broadcast_to(
                    regime[pl.ds(mine * rows + i, 1), :], (depth, lanes)
                )
                span = slice(half * lanes, (half + 1) * lanes)
                picked = product[:depth, span]
                for member in range(1, nreg):
                    part = product[member * depth : (member + 1) * depth, span]
                    picked = jnp.where(chosen == member, part, picked)
                value = picked * scale
                if n > 0:
                    value = value - shift * fields[n - 1, i + 1]
                fields[n, i + 1] = value
                packed = jnp.where(lane == i, pltpu.roll(value, i, 1), packed)
                packed = jnp.where(
                    lane == rows + i, pltpu.roll(value, lax.rem(rows + i + 1, lanes), 1), packed
                )
            edges[n] = packed
            return carry

        turns = piece // (2 * UNROLL_M)
        for chunk in chunks:
            if n == 0:
                slab_wait(0, chunk)

            def turn(t, carry, chunk=chunk):
                for u in range(UNROLL_M):
                    body(chunk * (piece // 2) + t * UNROLL_M + u, carry)
                return carry

            lax.fori_loop(0, turns, turn, 0)
        if not done:
            return
        for at, (sends, _, source, target, device) in enumerate(halo(n)):

            @pl.when(sends)
            def _(at=at, source=source, target=target, device=device):
                halo_copy(n, at, source, target, device).start()

    def halo_wait(n):
        for at, (_, gets, source, target, device) in enumerate(halo(n)):

            @pl.when(gets)
            def _(at=at, source=source, target=target, device=device):
                halo_copy(n, at, source, target, device).wait_recv()

    def fold(product):
        return jnp.sum(product.reshape(depth // 8, 8, lanes), axis=0)

    def operate(n):
        halo_wait(n)

        def body(i, carry):
            field = fields[n, i + 1]
            if n == 0:
                bulk = diag_z.reshape(depth * rows, lanes)[pl.ds(i, depth, stride=rows), :]
                diag_t[i] = bulk
            else:
                bulk = diag_t[i]
            beside = fields[n, i] + fields[n, i + 2]
            beside = beside + jnp.where(layer == 0, 0.0, pltpu.roll(field, 1, 0))
            beside = beside + jnp.where(layer == depth - 1, 0.0, pltpu.roll(field, depth - 1, 0))
            from_left = pltpu.roll(edges_left[n], lanes - rows - i, 1)
            beside = beside + jnp.where(lane == 0, from_left, pltpu.roll(field, 1, 1))
            from_right = pltpu.roll(edges_right[n], lanes - 1 - i, 1)
            beside = beside + jnp.where(
                lane == lanes - 1, from_right, pltpu.roll(field, lanes - 1, 1)
            )
            image = (6.0 + bulk) * field - beside
            images[n, i] = image
            sums = [fold(rhs_t[i] * field), fold(field * image)]
            for m in range(n):
                sums.append(fold(fields[m, i + 1] * image))
            return tuple(old + new for old, new in zip(carry, sums))

        start = tuple(jnp.zeros((8, lanes), jnp.float32) for _ in range(n + 2))
        parts = start
        for chunk in range(CHUNKS):
            if n == 0:
                slab_wait(1, chunk)

            def turn(t, carry, chunk=chunk):
                for u in range(UNROLL_A):
                    carry = body(chunk * piece + t * UNROLL_A + u, carry)
                return carry

            parts = lax.fori_loop(0, piece // UNROLL_A, turn, parts)
            if n == 0:
                precondition(1, [chunk], chunk == CHUNKS - 1)
        return [jnp.sum(part, axis=0, keepdims=True) for part in parts]

    everything = list(range(CHUNKS))
    precondition(0, everything, True)
    sums = operate(0)
    sums = sums + operate(1)
    precondition(2, everything, True)
    sums = sums + operate(2)

    sums.append(jnp.zeros((SUMS - len(sums), lanes), jnp.float32))
    value = jnp.concatenate(sums, axis=0)
    stages = (("gz", nz, mz, sums_z), ("gx", nx, mx, sums_x), ("gy", ny, my, sums_y))
    for stage, (name, count, me, slots) in enumerate(stages):
        slots[me] = value

        def sum_copy(k, peer, owner):
            return pltpu.make_async_remote_copy(
                src_ref=slots.at[me],
                dst_ref=slots.at[owner],
                send_sem=sum_send.at[stage, k],
                recv_sem=sum_recv.at[stage, k],
                device_id={name: peer},
                device_id_type=MESH,
            )

        for k in range(1, count):
            sum_copy(k, lax.rem(me + k, count), me).start()
        for k in range(1, count):
            sender = lax.rem(me + count - k, count)
            sum_copy(k, sender, sender).wait_recv()
        value = slots[0]
        for at in range(1, count):
            value = value + slots[at]
        for k in range(1, count):
            sum_copy(k, lax.rem(me + k, count), me).wait_send()

    def entry(at):
        row = jnp.sum(value[at : at + 1, :], axis=1, keepdims=True)
        return jnp.broadcast_to(row, (8, lanes))

    g0, a00, g1, a11, a01, g2, a22, a02, a12 = [entry(at) for at in range(9)]

    def inverse(pivot, size):
        good = pivot > 1e-7 * size
        return jnp.where(good, 1.0 / jnp.where(good, pivot, 1.0), 0.0)

    p0 = inverse(a00, a00)
    l1, l2 = a01 * p0, a02 * p0
    d1 = a11 - l1 * a01
    e1 = a12 - l2 * a01
    h1 = g1 - l1 * g0
    p1 = inverse(d1, a11)
    l21 = e1 * p1
    d2 = a22 - l2 * a02 - l21 * e1
    h2 = g2 - l2 * g0 - l21 * h1
    c2 = h2 * inverse(d2, a22)
    c1 = (h1 - e1 * c2) * p1
    c0 = (g0 - a01 * c1 - a02 * c2) * p0
    c0, c1, c2 = (c[0:1] for c in (c0, c1, c2))

    def mix(terms):
        first, second, third = terms
        return c0 * first + c1 * second + c2 * third

    x_rim[0] = mix([fields[n, 0] for n in range(BASIS)])
    x_rim[1] = mix([fields[n, rows + 1] for n in range(BASIS)])
    x_rim[2] = mix([edges_left[n] for n in range(BASIS)])
    x_rim[3] = mix([edges_right[n] for n in range(BASIS)])
    x_z[0] = jnp.zeros((rows, lanes), jnp.float32)
    x_z[depth + 1] = jnp.zeros((rows, lanes), jnp.float32)

    def rim_out(k, peer, owner):
        return pltpu.make_async_remote_copy(
            src_ref=x_rim.at[:, slab_span(peer), :],
            dst_ref=rim_in.at[owner],
            send_sem=rim_send.at[k],
            recv_sem=rim_recv.at[k],
            device_id={"gz": peer},
            device_id_type=MESH,
        )

    def slab_out(chunk, k, peer, owner):
        return pltpu.make_async_remote_copy(
            src_ref=x_z.at[pl.ds(peer * slab, slab + 2), pl.ds(chunk * piece, piece), :],
            dst_ref=x_in.at[owner, :, pl.ds(chunk * piece, piece), :],
            send_sem=out_send.at[chunk, k],
            recv_sem=out_recv.at[chunk, k],
            device_id={"gz": peer},
            device_id_type=MESH,
        )

    for chunk in range(CHUNKS):

        def final(t, carry):
            for u in range(UNROLL_F):
                i = chunk * piece + t * UNROLL_F + u
                x = mix([fields[n, i + 1] for n in range(BASIS)])
                x_z.reshape((depth + 2) * rows, lanes)[pl.ds(rows + i, depth, stride=rows), :] = x
            return carry

        lax.fori_loop(0, piece // UNROLL_F, final, 0)
        for k in range(1, nz):
            slab_out(chunk, k, lax.rem(mz + k, nz), mz).start()
    for k in range(1, nz):
        rim_out(k, lax.rem(mz + k, nz), mz).start()

    own_x = pltpu.make_async_copy(
        x_z.at[pl.ds(mz * slab, slab + 2)], x_in.at[mz], local_sem.at[0]
    )
    own_rim = pltpu.make_async_copy(
        x_rim.at[:, slab_span(mz), :], rim_in.at[mz], local_sem.at[1]
    )
    own_x.start()
    own_rim.start()
    for which, (source, target) in enumerate(slabs):
        pltpu.make_async_copy(source, target, slab_sem.at[which]).wait()
    for which in range(2):
        for chunk in range(CHUNKS):
            for k in range(1, nz):
                slab_in(which, chunk, k, lax.rem(mz + k, nz), mz).wait_send()
    for n in range(BASIS):
        for at, (sends, _, source, target, device) in enumerate(halo(n)):

            @pl.when(sends)
            def _(n=n, at=at, source=source, target=target, device=device):
                halo_copy(n, at, source, target, device).wait_send()

    plane_lane = lax.broadcasted_iota(jnp.int32, (rows, lanes), 1)
    plane_row = lax.broadcasted_iota(jnp.int32, (rows, lanes), 0)

    def result(which, owner):
        source = x_in.at[owner, pl.ds(1, slab)] if which == 0 else r_in.at[owner]
        return pltpu.make_async_copy(
            source,
            (x_out, r_out)[which].at[:, row_span(owner, 0, rows), :],
            out_local.at[which, owner],
        )

    def finish(owner):
        result(0, owner).start()
        rim = [rim_in[owner, 2], rim_in[owner, 3]]
        rim.append(jnp.zeros((lanes - 2 * slab, lanes), jnp.float32))
        turned = jnp.concatenate(rim, axis=0).T
        first, last = turned[rows : 2 * rows], turned[:rows]
        start = pl.multiple_of(place(owner) * rows, 8)

        def plane(z, carry):
            x = x_in[owner, z + 1]
            beside = x_in[owner, z] + x_in[owner, z + 2]
            above = jnp.broadcast_to(rim_in[owner, 0, pl.ds(z, 1), :], x.shape)
            below = jnp.broadcast_to(rim_in[owner, 1, pl.ds(z, 1), :], x.shape)
            beside = beside + jnp.where(plane_row == 0, above, pltpu.roll(x, 1, 0))
            beside = beside + jnp.where(plane_row == rows - 1, below, pltpu.roll(x, rows - 1, 0))
            from_left = pltpu.roll(first, lax.rem(lanes - z, lanes), 1)
            from_right = pltpu.roll(last, lanes - 1 - slab - z, 1)
            beside = beside + jnp.where(plane_lane == 0, from_left, pltpu.roll(x, 1, 1))
            beside = beside + jnp.where(
                plane_lane == lanes - 1, from_right, pltpu.roll(x, lanes - 1, 1)
            )
            image = (6.0 + diag_slab[z, pl.ds(start, rows), :]) * x - beside
            r_in[owner, z] = rhs_slab[z, pl.ds(start, rows), :] - image
            return carry

        def turn(t, carry):
            for u in range(UNROLL_F):
                carry = plane(t * UNROLL_F + u, carry)
            return carry

        lax.fori_loop(0, slab // UNROLL_F, turn, 0)
        result(1, owner).start()

    own_x.wait()
    own_rim.wait()
    finish(mz)
    order = sorted(range(1, nz), key=lambda k: (min(k, nz - k), k))
    for k in order:
        sender = lax.rem(mz + nz - k, nz)
        rim_out(k, sender, sender).wait_recv()
        for chunk in range(CHUNKS):
            slab_out(chunk, k, sender, sender).wait_recv()
        finish(sender)
    for k in range(nz):
        for which in range(2):
            result(which, lax.rem(mz + k, nz)).wait()
    for k in range(1, nz):
        peer = lax.rem(mz + k, nz)
        rim_out(k, peer, mz).wait_send()
        for chunk in range(CHUNKS):
            slab_out(chunk, k, peer, mz).wait_send()


def per_device(sizes, right_side, diagonal, regime, inverses):
    slab, wide, lanes = right_side.shape
    nz = sizes["gz"]
    depth, rows = slab * nz, wide // nz
    nreg = inverses.shape[0]
    column = (rows, depth, lanes)
    layered = (depth, rows, lanes)
    f32 = jnp.float32
    dma = pltpu.SemaphoreType.DMA
    return pl.pallas_call(
        functools.partial(kernel, sizes),
        out_shape=[jax.ShapeDtypeStruct(right_side.shape, f32)] * 2,
        in_specs=[pl.BlockSpec(memory_space=pl.ANY)] * 2
        + [pl.BlockSpec(memory_space=pltpu.VMEM)] * 2,
        out_specs=[pl.BlockSpec(memory_space=pl.ANY)] * 2,
        scratch_shapes=[
            pltpu.VMEM((nreg * depth, 3 * depth), jnp.bfloat16),
            pltpu.VMEM(layered, f32),
            pltpu.VMEM(layered, f32),
            pltpu.VMEM(right_side.shape, f32),
            pltpu.VMEM(right_side.shape, f32),
            pltpu.VMEM(column, f32),
            pltpu.VMEM(column, f32),
            pltpu.VMEM((BASIS, rows + 2, depth, lanes), f32),
            pltpu.VMEM((BASIS, rows, depth, lanes), f32),
            pltpu.VMEM((BASIS, depth, lanes), f32),
            pltpu.VMEM((BASIS, depth, lanes), f32),
            pltpu.VMEM((BASIS, depth, lanes), f32),
            pltpu.VMEM((depth + 2, rows, lanes), f32),
            pltpu.VMEM((4, depth, lanes), f32),
            pltpu.VMEM((nz, slab + 2, rows, lanes), f32),
            pltpu.VMEM((nz, 4, slab, lanes), f32),
            pltpu.VMEM((nz, slab, rows, lanes), f32),
            pltpu.VMEM((nz, SUMS, lanes), f32),
            pltpu.VMEM((sizes["gx"], SUMS, lanes), f32),
            pltpu.VMEM((sizes["gy"], SUMS, lanes), f32),
            dma((2,)),
            dma((2, CHUNKS, nz)),
            dma((2, CHUNKS, nz)),
            dma((BASIS, 4)),
            dma((BASIS, 4)),
            dma((3, max(sizes.values()))),
            dma((3, max(sizes.values()))),
            dma((CHUNKS, nz)),
            dma((CHUNKS, nz)),
            dma((2, nz)),
            dma((nz,)),
            dma((nz,)),
            dma((2,)),
        ],
        compiler_params=pltpu.CompilerParams(
            collective_id=0, has_side_effects=True, vmem_limit_bytes=56 * 1024 * 1024
        ),
    )(right_side, diagonal, regime, inverses)


def solution(mesh):
    sizes = {name: mesh.shape[name] for name in ("gx", "gy", "gz")}
    in_specs = (P("gz", "gx", "gy"), P("gz", "gx", "gy"), P("gx", "gy"), P())
    out_specs = (P("gz", "gx", "gy"), P("gz", "gx", "gy"))
    return jax.shard_map(
        functools.partial(per_device, sizes),
        mesh=mesh,
        in_specs=in_specs,
        out_specs=out_specs,
        check_vma=False,
    )
```
